32 devices in a mesh: lat: 4 (over x, core), lon: 8 (over z, y).
Axes of the slice: x: 2, y: 2, z: 4, core: 2. Of those that a mesh axis runs over, the one named last changes fastest.
Arguments:
- tokens: bfloat16 [4, 48, 96, 512], P(None, 'lat', 'lon'), may hold values from -6 to 6
- region: int32 [4, 48, 96], P(None, 'lat', 'lon'), may hold values from 0 to 2
- norm_gain1: float32 [2, 512], replicated, may hold values from 0.25 to 1.75
- qkv_weight: bfloat16 [2, 512, 1536], replicated, may hold values from -3 to 3
- proj_weight: bfloat16 [2, 512, 512], replicated, may hold values from -0.25 to 0.25
- norm_gain2: float32 [2, 512], replicated, may hold values from 0.25 to 1.75
- up_weight: bfloat16 [2, 512, 2048], replicated, may hold values from -0.25 to 0.25
- down_weight: bfloat16 [2, 2048, 512], replicated, may hold values from -0.125 to 0.125
Outputs:
- result: bfloat16 [4, 48, 96, 512], P(None, 'lat', 'lon')
The draws below stay inside these ranges and needn't reach their ends.
All inputs are finite; a program needn't handle non-finite values.
Results may differ from the reference program's by a relative error of at most 0.012.
Values may be sent and summed in bfloat16 or wider, within the bound.
A program may use at most 64 MiB of HBM per device.

```python
import math
import jax
import jax.numpy as jnp
from jax import lax

D = 512
FF = 2048
HEADS = 8
LEV = 4
WLEV = 2
WLAT = 6
WLON = 12
NLAT = 48
NLON = 96


def draw_qkv_weight(key, part):
    first_key = jax.random.fold_in(jax.random.fold_in(key, 17), 0)
    base = jax.random.normal(first_key, (2, D, 3 * D), jnp.float32) / math.sqrt(D)
    return base.astype(jnp.bfloat16)


def plant(values, key, least, largest):
    longest = values.shape.index(max(values.shape))
    spots = []
    for shift in (0, 1):
        where = [jax.random.randint(jax.random.fold_in(key, axis), (), 0, length) for axis, length in enumerate(values.shape)]
        where[longest] = (where[longest] + shift) % values.shape[longest]
        spots.append(tuple(where))
    return values.at[spots[0]].set(least).at[spots[1]].set(largest)


def block_levels(rng, shape, cuts, low, largest):
    factor_of, own = 1.0, jax.random.fold_in(rng, 6)
    for axis_at, parts in cuts:
        steps = jnp.exp(jax.random.uniform(jax.random.fold_in(own, axis_at), (parts,), jnp.float32, low / len(cuts), largest / len(cuts)))
        factor_of = factor_of * jnp.repeat(steps, shape[axis_at] // parts).reshape([-1 if axis == axis_at else 1 for axis in range(len(shape))])
    return factor_of


def bell_draw(key, extent, scale, limit, cuts=(), held_as=jnp.bfloat16):
    drawn = jax.random.normal(key, extent, jnp.float32) * scale
    if len(cuts) > 0:
        drawn = block_levels(key, extent, cuts, -0.22, 0.18) * drawn
    return jnp.clip(drawn, min=-limit, max=limit).astype(held_as)


def setup_inputs(seed: int = 0) -> dict:
    splits = jax.random.split(jax.random.key(seed), 9)
    tokens = bell_draw(splits[0], (LEV, NLAT, NLON, D), 1.0, 6.0, ((1, 4), (2, 8)))
    region = plant(jax.random.randint(splits[1], (LEV, NLAT, NLON), 0, 3), jax.random.fold_in(splits[1], 1), 0, 2).astype(jnp.int32)
    norm_gain1 = jnp.clip(1.0 + 0.15 * jax.random.normal(splits[2], (2, D), jnp.float32), 0.25, 1.75)
    qkv_weight = draw_qkv_weight(jax.random.fold_in(splits[8], 71), 0)
    proj_weight = bell_draw(splits[4], (2, D, D), D ** -0.5, 0.25)
    norm_gain2 = jnp.clip(1.0 + 0.15 * jax.random.normal(splits[5], (2, D), jnp.float32), 0.25, 1.75)
    up_weight = bell_draw(splits[6], (2, D, FF), D ** -0.5, 0.25)
    down_weight = bell_draw(splits[7], (2, FF, D), FF ** -0.5, 0.125)
    return {"tokens": tokens, "region": region, "norm_gain1": norm_gain1, "qkv_weight": qkv_weight, "proj_weight": proj_weight, "norm_gain2": norm_gain2, "up_weight": up_weight, "down_weight": down_weight}


epsilon = 1e-05

def layer_norm(field, gain_vector):
    field = field.astype(jnp.float32)
    average = lax.optimization_barrier(jnp.mean(field, axis=-1, keepdims=True))
    centered = field - average
    variance = lax.optimization_barrier(jnp.mean(centered * centered, axis=-1, keepdims=True))
    return centered * lax.rsqrt(variance + epsilon) * gain_vector

def to_windows(field):
    level_count, row_count, column_count = field.shape[:3]
    trailing = tuple(field.shape[3:])
    shaped = field.reshape((level_count // WLEV, WLEV, row_count // WLAT, WLAT, column_count // WLON, WLON) + trailing)
    order = (0, 2, 4, 1, 3, 5) + tuple(range(6, 6 + len(trailing)))
    return jnp.transpose(shaped, order).reshape((-1, WLEV * WLAT * WLON) + trailing)

def from_windows(windows, level_count, row_count, column_count):
    trailing = tuple(windows.shape[2:])
    shaped = windows.reshape((level_count // WLEV, row_count // WLAT, column_count // WLON, WLEV, WLAT, WLON) + trailing)
    order = (0, 3, 1, 4, 2, 5) + tuple(range(6, 6 + len(trailing)))
    return jnp.transpose(shaped, order).reshape((level_count, row_count, column_count) + trailing)

def window_attention(normed, labels, w_qkv, w_proj):
    count, span, features = normed.shape
    head_size = features // HEADS
    mixed = jnp.dot(normed, w_qkv, preferred_element_type=jnp.float32).astype(jnp.bfloat16)
    queries = mixed[..., :features].reshape(count, span, HEADS, head_size).astype(jnp.float32)
    key_vectors = mixed[..., features:2 * features].reshape(count, span, HEADS, head_size).astype(jnp.float32)
    values = mixed[..., 2 * features:].reshape(count, span, HEADS, head_size).astype(jnp.float32)
    scores = jnp.einsum('wqhd,wkhd->whqk', queries, key_vectors) * (1.0 / math.sqrt(head_size))
    allowed = labels[:, None, :, None] == labels[:, None, None, :]
    scores = jnp.where(allowed, scores, -jnp.inf)
    peak = lax.optimization_barrier(jnp.max(scores, axis=-1, keepdims=True))
    exponent = jnp.exp(scores - peak)
    attention_weights = (exponent / lax.optimization_barrier(jnp.sum(exponent, axis=-1, keepdims=True))).astype(jnp.bfloat16)
    gathered = jnp.einsum('whqk,wkhd->wqhd', attention_weights.astype(jnp.float32), values)
    gathered = gathered.astype(jnp.bfloat16).reshape(count, span, features)
    return jnp.dot(gathered, w_proj, preferred_element_type=jnp.float32)

def attention_part(field, labels, gain_vector, w_qkv, w_proj):
    level_count, row_count, column_count, features = field.shape
    normed = layer_norm(field, gain_vector).astype(jnp.bfloat16)
    windows = to_windows(normed)
    window_labels = to_windows(labels)
    per_row = column_count // WLON
    groups = windows.reshape((-1, per_row) + tuple(windows.shape[1:]))
    label_groups = window_labels.reshape((-1, per_row) + tuple(window_labels.shape[1:]))

    def attend(pair):
        return window_attention(pair[0], pair[1], w_qkv, w_proj)
    projected = lax.map(attend, (groups, label_groups)).reshape(windows.shape)
    return field.astype(jnp.float32) + from_windows(projected, level_count, row_count, column_count)

def feed_forward(field, gain_vector, w_up, w_down):

    def per_level(level_field):
        normed = layer_norm(level_field, gain_vector).astype(jnp.bfloat16)
        hidden_units = jax.nn.gelu(jnp.dot(normed, w_up, preferred_element_type=jnp.float32)).astype(jnp.bfloat16)
        return (level_field + jnp.dot(hidden_units, w_down, preferred_element_type=jnp.float32)).astype(jnp.bfloat16)
    return lax.map(per_level, field)

def reference(tokens, region, norm_gain1, qkv_weight, proj_weight, norm_gain2, up_weight, down_weight):
    half_level = WLEV // 2
    half_row = WLAT // 2
    half_column = WLON // 2
    mixed_first = attention_part(tokens, region, norm_gain1[0], qkv_weight[0], proj_weight[0])
    first_out = feed_forward(mixed_first, norm_gain2[0], up_weight[0], down_weight[0])
    rolled = jnp.roll(first_out, (-half_level, -half_row, -half_column), (0, 1, 2))
    rolled_region = jnp.roll(region, (-half_level, -half_row, -half_column), (0, 1, 2))
    level_index = jnp.arange(LEV, dtype=jnp.int32)[:, None, None]
    row_index = jnp.arange(NLAT, dtype=jnp.int32)[None, :, None]
    wrapped_level = (level_index >= LEV - half_level).astype(jnp.int32)
    wrapped_row = (row_index >= NLAT - half_row).astype(jnp.int32)
    labels_second = rolled_region * 4 + wrapped_level * 2 + wrapped_row
    mixed_second = attention_part(rolled, labels_second, norm_gain1[1], qkv_weight[1], proj_weight[1])
    restored = jnp.roll(mixed_second, (half_level, half_row, half_column), (0, 1, 2))
    return feed_forward(restored, norm_gain2[1], up_weight[1], down_weight[1])
```

```python
import functools

import jax
import jax.numpy as jnp
from jax import lax
from jax.experimental import pallas as pl
from jax.experimental.pallas import tpu as pltpu
from jax.sharding import PartitionSpec as P

HEADS = 8
WLEV = 2
WLAT = 6
WLON = 12
EPSILON = 1e-05
FAR = -1e30
MESH = pl.DeviceIdType.MESH
F32 = jnp.float32
BF16 = jnp.bfloat16


def normed(field, gain):
    mean = jnp.mean(field, axis=-1, keepdims=True)
    centered = field - mean
    variance = jnp.mean(centered * centered, axis=-1, keepdims=True)
    return (centered * lax.rsqrt(variance + EPSILON) * gain).astype(BF16)


def gelu(x):
    inner = x * (0.7978845608028654 + 0.035677408136300125 * (x * x))
    half = 0.5 * x
    return half + half * jnp.tanh(inner)


def dot(a, b):
    return jnp.dot(a, b, preferred_element_type=F32)


def dot_t(a, b):
    return lax.dot_general(a, b, (((1,), (1,)), ((), ())), preferred_element_type=F32)


def kernel(
    x_ref, e_ref, g1_ref, g2_ref, wqkv_hbm, wproj_hbm, wup_hbm, wdown_hbm, out_ref,
    own, shift, back, eshift, xin, qkv, heads, bias,
    wqkv, wproj, wup, wdown, wsem, fsend, frecv, bsend, brecv, esend, erecv,
):
    lat_count, lon_count = lax.axis_size("lat"), lax.axis_size("lon")
    lat, lon = lax.axis_index("lat"), lax.axis_index("lon")
    up = lax.rem(lat + lat_count - 1, lat_count)
    down = lax.rem(lat + 1, lat_count)
    left = lax.rem(lon + lon_count - 1, lon_count)
    right = lax.rem(lon + 1, lon_count)
    before = {"left": (lat, left), "up": (up, lon), "corner": (up, left)}
    after = {"left": (lat, right), "up": (down, lon), "corner": (down, right)}

    weights = []
    for block in range(2):
        for at, (source, target) in enumerate(
            ((wqkv_hbm, wqkv), (wproj_hbm, wproj), (wup_hbm, wup), (wdown_hbm, wdown))
        ):
            copy = pltpu.make_async_copy(
                source.at[block], target.at[block], wsem.at[block * 4 + at]
            )
            copy.start()
            weights.append(copy)

    barrier = pltpu.get_barrier_semaphore()
    for device in list(before.values()) + list(after.values()):
        pl.semaphore_signal(barrier, inc=1, device_id=device, device_id_type=MESH)
    pl.semaphore_wait(barrier, 6)

    moves = (
        (2, 0, 1, "left"),
        (4, 0, 3, "left"),
        (6, 1, 1, "left"),
        (1, 1, 2, "up"),
        (0, 1, 3, "corner"),
    )

    def label_copy(at):
        atom, window, place, towards = moves[at]
        return pltpu.make_async_remote_copy(
            e_ref.at[atom], eshift.at[window, place], esend.at[at], erecv.at[at],
            device_id=before[towards], device_id_type=MESH,
        )

    def forward_copy(at):
        atom, window, place, towards = moves[at]
        return pltpu.make_async_remote_copy(
            own.at[atom], shift.at[window, place], fsend.at[at], frecv.at[at],
            device_id=before[towards], device_id_type=MESH,
        )

    def backward_copy(at):
        atom, window, place, towards = moves[at]
        return pltpu.make_async_remote_copy(
            back.at[window, place], out_ref.at[atom], bsend.at[at], brecv.at[at],
            device_id=after[towards], device_id_type=MESH,
        )

    for at in range(5):
        label_copy(at).start()

    span, features = xin.shape
    atom_size = span // 4
    pair = 128
    lane = lax.broadcasted_iota(jnp.int32, (1, pair), 1)
    low = lane < 64
    scale = 64 ** -0.5
    head_masks = (
        jnp.where(low, scale, 0.0).astype(BF16),
        jnp.where(low, 0.0, scale).astype(BF16),
    )

    def set_bias(marks, block):
        half = low if block == 0 else jnp.logical_not(low)
        query = (marks * jnp.where(half, FAR, 0.0)).astype(BF16)
        key = (1.0 - marks).astype(BF16)
        bias[...] = dot_t(query, key)

    def unit(x, block, waits):
        if waits:
            weights[block * 4].wait()
        qkv[...] = dot(normed(x, g1_ref[block : block + 1, :]), wqkv[block]).astype(BF16)
        ones = jnp.ones((span, pair), BF16)
        for at in range(features // pair):
            cols = slice(at * pair, (at + 1) * pair)
            query = qkv[:, cols]
            key = qkv[:, features + at * pair : features + (at + 1) * pair]
            value = qkv[:, 2 * features + at * pair : 2 * features + (at + 1) * pair]
            value = jnp.concatenate([value, ones], axis=1)
            parts = []
            for mask in head_masks:
                scores = dot_t(query * mask, key) + bias[...]
                peak = jnp.max(scores, axis=-1, keepdims=True)
                weight = jnp.exp(scores - peak).astype(BF16)
                total = dot(weight, value)
                parts.append(total[:, :pair] / total[:, pair:])
            heads[:, cols] = jnp.where(low, parts[0], parts[1]).astype(BF16)
        if waits:
            weights[block * 4 + 1].wait()
        h = x + dot(heads[...], wproj[block])
        n2 = normed(h, g2_ref[block : block + 1, :])
        if waits:
            weights[block * 4 + 2].wait()
            weights[block * 4 + 3].wait()
        hidden = wup.shape[2]
        step = 512
        for at in range(hidden // step):
            cols = slice(at * step, (at + 1) * step)
            inner = gelu(dot(n2, wup[block, :, cols])).astype(BF16)
            h = h + dot(inner, wdown[block, cols, :])
        return h

    def rows(ref, first):
        return jnp.concatenate([ref[first + at].astype(F32) for at in range(4)], axis=0)

    for u in range(2):
        set_bias(rows(e_ref, 4 * u), 0)
        h = unit(rows(x_ref, 4 * u), 0, u == 0)
        for at in range(4):
            own[4 * u + at] = h[at * atom_size : (at + 1) * atom_size].astype(BF16)
        for at, move in enumerate(moves):
            if move[0] // 4 == u:
                forward_copy(at).start()

    local = {(0, 0): 3, (0, 2): 5, (1, 0): 7}
    arrivals = {(move[1], move[2]): at for at, move in enumerate(moves)}
    for w in range(2):
        for place in range(4):
            if (w, place) in arrivals:
                label_copy(arrivals[w, place]).wait_recv()
                forward_copy(arrivals[w, place]).wait_recv()
        marks = jnp.concatenate(
            [
                (e_ref[local[w, place]] if (w, place) in local else eshift[w, place]).astype(F32)
                for place in range(4)
            ],
            axis=0,
        )
        set_bias(marks, 1)
        x = jnp.concatenate(
            [
                (own[local[w, place]] if (w, place) in local else shift[w, place]).astype(F32)
                for place in range(4)
            ],
            axis=0,
        )
        h = unit(x, 1, w == 0)
        for place in range(4):
            piece = h[place * atom_size : (place + 1) * atom_size].astype(BF16)
            if (w, place) in local:
                out_ref[local[w, place]] = piece
            else:
                back[w, place] = piece
        for at, move in enumerate(moves):
            if move[1] == w:
                backward_copy(at).start()
    for at in range(5):
        backward_copy(at).wait_recv()
    for at in range(5):
        label_copy(at).wait_send()
        forward_copy(at).wait_send()
        backward_copy(at).wait_send()


def to_atoms(field):
    levels, row_count, column_count = field.shape[:3]
    trailing = tuple(field.shape[3:])
    half_row, half_column = WLAT // 2, WLON // 2
    shaped = field.reshape(
        (levels, row_count // half_row, half_row, column_count // half_column, half_column)
        + trailing
    )
    order = (1, 3, 0, 2, 4) + tuple(range(5, 5 + len(trailing)))
    return jnp.transpose(shaped, order).reshape(
        (-1, levels * half_row * half_column) + trailing
    )


def from_atoms(atoms, levels, row_count, column_count):
    trailing = tuple(atoms.shape[2:])
    half_row, half_column = WLAT // 2, WLON // 2
    shaped = atoms.reshape(
        (row_count // half_row, column_count // half_column, levels, half_row, half_column)
        + trailing
    )
    order = (2, 0, 3, 1, 4) + tuple(range(5, 5 + len(trailing)))
    return jnp.transpose(shaped, order).reshape((levels, row_count, column_count) + trailing)


def per_device(
    tokens, region, norm_gain1, qkv_weight, proj_weight, norm_gain2, up_weight, down_weight
):
    levels, row_count, column_count, features = tokens.shape
    hidden = up_weight.shape[2]
    x = to_atoms(tokens)
    atoms, size, _ = x.shape
    span = 4 * size

    level = jnp.arange(levels, dtype=jnp.int32)[:, None, None]
    row = (lax.axis_index("lat") * row_count + jnp.arange(row_count, dtype=jnp.int32))[None, :, None]
    pair_first = level // WLEV
    rolled_level = (level + levels - WLEV // 2) % levels
    wrapped_level = (rolled_level >= levels - WLEV // 2).astype(jnp.int32)
    wrapped_row = (row < WLAT // 2).astype(jnp.int32)
    first_class = region * 2 + pair_first
    second_class = ((region * 2 + rolled_level // WLEV) * 2 + wrapped_level) * 2 + wrapped_row
    classes = jnp.stack([first_class, second_class + 64], axis=-1)
    classes = to_atoms(classes)
    lane = jnp.arange(128, dtype=jnp.int32)
    marks = (
        (classes[:, :, :1] == lane) | (classes[:, :, 1:] == lane)
    ).astype(BF16)

    vmem = pl.BlockSpec(memory_space=pltpu.VMEM)
    hbm = pl.BlockSpec(memory_space=pl.ANY)
    out = pl.pallas_call(
        kernel,
        out_shape=jax.ShapeDtypeStruct((atoms, size, features), BF16),
        in_specs=[vmem] * 4 + [hbm] * 4,
        out_specs=vmem,
        scratch_shapes=[
            pltpu.VMEM((atoms, size, features), BF16),
            pltpu.VMEM((2, 4, size, features), BF16),
            pltpu.VMEM((2, 4, size, features), BF16),
            pltpu.VMEM((2, 4, size, 128), BF16),
            pltpu.VMEM((span, features), F32),
            pltpu.VMEM((span, 3 * features), BF16),
            pltpu.VMEM((span, features), BF16),
            pltpu.VMEM((span, span), F32),
            pltpu.VMEM(qkv_weight.shape, BF16),
            pltpu.VMEM(proj_weight.shape, BF16),
            pltpu.VMEM(up_weight.shape, BF16),
            pltpu.VMEM(down_weight.shape, BF16),
            pltpu.SemaphoreType.DMA((8,)),
            pltpu.SemaphoreType.DMA((5,)),
            pltpu.SemaphoreType.DMA((5,)),
            pltpu.SemaphoreType.DMA((5,)),
            pltpu.SemaphoreType.DMA((5,)),
            pltpu.SemaphoreType.DMA((5,)),
            pltpu.SemaphoreType.DMA((5,)),
        ],
        compiler_params=pltpu.CompilerParams(
            collective_id=0, has_side_effects=True, vmem_limit_bytes=50 * 1024 * 1024
        ),
    )(x, marks, norm_gain1, norm_gain2, qkv_weight, proj_weight, up_weight, down_weight)
    return from_atoms(out, levels, row_count, column_count)


def solution(mesh):
    return jax.shard_map(
        per_device,
        mesh=mesh,
        in_specs=(P(None, "lat", "lon", None), P(None, "lat", "lon"), P(), P(), P(), P(), P(), P()),
        out_specs=P(None, "lat", "lon", None),
        check_vma=False,
    )
```

```python
import functools

import jax
import jax.numpy as jnp
from jax import lax
from jax.experimental import pallas as pl
from jax.experimental.pallas import tpu as pltpu
from jax.sharding import PartitionSpec as P

HEADS = 8
WLEV = 2
WLAT = 6
WLON = 12
EPSILON = 1e-05
FAR = -1e30
MESH = pl.DeviceIdType.MESH
F32 = jnp.float32
BF16 = jnp.bfloat16


def normed(field, gain):
    mean = jnp.mean(field, axis=-1, keepdims=True)
    centered = field - mean
    variance = jnp.mean(centered * centered, axis=-1, keepdims=True)
    return (centered * lax.rsqrt(variance + EPSILON) * gain).astype(BF16)


def gelu(x):
    inner = x * (0.7978845608028654 + 0.035677408136300125 * (x * x))
    half = 0.5 * x
    return half + half * jnp.tanh(inner)


def dot(a, b):
    return jnp.dot(a, b, preferred_element_type=F32)


def dot_t(a, b):
    return lax.dot_general(a, b, (((1,), (1,)), ((), ())), preferred_element_type=F32)


def kernel(
    x_ref, e_ref, g1_ref, g2_ref, wqkv_hbm, wproj_hbm, wup_hbm, wdown_hbm, out_ref,
    own, shift, back, eshift, xs, qkv, heads, bias,
    wqkv, wproj, wup, wdown, wsem, fsend, frecv, bsend, brecv, esend, erecv,
):
    lat_count, lon_count = lax.axis_size("lat"), lax.axis_size("lon")
    lat, lon = lax.axis_index("lat"), lax.axis_index("lon")
    up = lax.rem(lat + lat_count - 1, lat_count)
    down = lax.rem(lat + 1, lat_count)
    left = lax.rem(lon + lon_count - 1, lon_count)
    right = lax.rem(lon + 1, lon_count)
    before = {"left": (lat, left), "up": (up, lon), "corner": (up, left)}
    after = {"left": (lat, right), "up": (down, lon), "corner": (down, right)}

    weights = [
        pltpu.make_async_copy(source.at[block], target.at[block], wsem.at[block * 4 + at])
        for block in range(2)
        for at, (source, target) in enumerate(
            ((wqkv_hbm, wqkv), (wproj_hbm, wproj), (wup_hbm, wup), (wdown_hbm, wdown))
        )
    ]
    weights[0].start()
    weights[1].start()

    barrier = pltpu.get_barrier_semaphore()
    for device in list(before.values()) + list(after.values()):
        pl.semaphore_signal(barrier, inc=1, device_id=device, device_id_type=MESH)

    moves = (
        (2, 0, 0, "left"),
        (0, 1, 1, "corner"),
        (4, 0, 1, "left"),
        (6, 1, 0, "left"),
        (1, 1, 2, "up"),
    )
    local = {(0, 2): 3, (0, 3): 5, (1, 3): 7}
    arrivals = {(move[1], move[2]): at for at, move in enumerate(moves)}

    def label_copy(at):
        atom, window, place, towards = moves[at]
        return pltpu.make_async_remote_copy(
            e_ref.at[atom], eshift.at[window, place], esend.at[at], erecv.at[at],
            device_id=before[towards], device_id_type=MESH,
        )

    def forward_copy(at):
        atom, window, place, towards = moves[at]
        return pltpu.make_async_remote_copy(
            own.at[atom], shift.at[window, place], fsend.at[at], frecv.at[at],
            device_id=before[towards], device_id_type=MESH,
        )

    def backward_copy(at):
        atom, window, place, towards = moves[at]
        return pltpu.make_async_remote_copy(
            back.at[window, place], out_ref.at[atom], bsend.at[at], brecv.at[at],
            device_id=after[towards], device_id_type=MESH,
        )

    span, features = xs.shape[1:]
    atom_size = span // 4
    part_size = span // 2
    pair = 128
    lane = lax.broadcasted_iota(jnp.int32, (1, pair), 1)
    low = lane < 64
    scale = 64 ** -0.5
    head_masks = (
        jnp.where(low, scale, 0.0).astype(BF16),
        jnp.where(low, 0.0, scale).astype(BF16),
    )

    def prepare(block, at, pieces, marks):
        index = 2 * block + at
        marks = jnp.concatenate([piece.astype(F32) for piece in marks], axis=0)
        half = low if block == 0 else jnp.logical_not(low)
        query = (marks * jnp.where(half, FAR, 0.0)).astype(BF16)
        bias[index] = dot_t(query, (1.0 - marks).astype(BF16))
        x = jnp.concatenate([piece.astype(F32) for piece in pieces], axis=0)
        xs[index] = x
        n1 = normed(x, g1_ref[block : block + 1, :])
        if at == 0:
            weights[block * 4].wait()
        qkv[index] = dot(n1, wqkv[block]).astype(BF16)

    def part(block, at, which, first):
        index = 2 * block + at
        rows = slice(which * part_size, (which + 1) * part_size)
        ones = jnp.ones((span, pair), BF16)
        offset = bias[index, rows, :]
        offset = jnp.concatenate([offset, offset], axis=0)
        for column in range(0, features, pair):
            query = qkv[index, rows, column : column + pair]
            key = qkv[index, :, features + column : features + column + pair]
            value = qkv[index, :, 2 * features + column : 2 * features + column + pair]
            value = jnp.concatenate([value, ones], axis=1)
            query = jnp.concatenate([query * head_masks[0], query * head_masks[1]], axis=0)
            scores = dot_t(query, key) + offset
            peak = jnp.max(scores, axis=-1, keepdims=True)
            weight = jnp.exp(scores - peak).astype(BF16)
            total = dot(weight, value)
            total = total[:, :pair] / total[:, pair:]
            heads[index, rows, column : column + pair] = jnp.where(
                low, total[:part_size], total[part_size:]
            ).astype(BF16)
        if first:
            weights[block * 4 + 1].wait()
        h = xs[index, rows, :] + dot(heads[index, rows, :], wproj[block])
        n2 = normed(h, g2_ref[block : block + 1, :])
        if first:
            weights[block * 4 + 2].wait()
            weights[block * 4 + 3].wait()
        hidden = wup.shape[2]
        step = 512
        for column in range(0, hidden, step):
            inner = gelu(dot(n2, wup[block, :, column : column + step])).astype(BF16)
            h = h + dot(inner, wdown[block, column : column + step, :])
        return h[:atom_size].astype(BF16), h[atom_size:].astype(BF16)

    def prepare_first(u):
        atoms = (4 * u, 4 * u + 2, 4 * u + 1, 4 * u + 3)
        prepare(0, u, [x_ref[a] for a in atoms], [e_ref[a] for a in atoms])

    def part_first(u, which, first=False):
        own[4 * u + which], own[4 * u + 2 + which] = part(0, u, which, first)

    prepare_first(0)
    weights[2].start()
    weights[3].start()
    part_first(0, 0, True)
    pl.semaphore_wait(barrier, 6)
    for at in range(5):
        label_copy(at).start()
    forward_copy(0).start()
    forward_copy(1).start()
    for at in range(4, 8):
        weights[at].start()
    prepare_first(1)
    part_first(1, 0)
    forward_copy(2).start()
    forward_copy(3).start()
    part_first(0, 1)
    forward_copy(4).start()
    part_first(1, 1)

    def prepare_second(w):
        pieces, marks = [], []
        for place in range(4):
            if (w, place) in arrivals:
                label_copy(arrivals[w, place]).wait_recv()
                forward_copy(arrivals[w, place]).wait_recv()
        for place in range(4):
            if (w, place) in arrivals:
                pieces.append(shift[w, place])
                marks.append(eshift[w, place])
            else:
                pieces.append(own[local[w, place]])
                marks.append(e_ref[local[w, place]])
        prepare(1, w, pieces, marks)

    def part_second(w, which, first=False):
        results = part(1, w, which, first)
        for at in range(2):
            place = 2 * which + at
            if (w, place) in local:
                out_ref[local[w, place]] = results[at]
            else:
                back[w, place] = results[at]
        for at in range(2):
            if (w, 2 * which + at) in arrivals:
                backward_copy(arrivals[w, 2 * which + at]).start()

    prepare_second(0)
    part_second(0, 0, True)
    prepare_second(1)
    part_second(1, 0)
    part_second(1, 1)
    part_second(0, 1)
    for at in range(5):
        backward_copy(at).wait_recv()
    for at in range(5):
        label_copy(at).wait_send()
        forward_copy(at).wait_send()
        backward_copy(at).wait_send()


def to_atoms(field):
    levels, row_count, column_count = field.shape[:3]
    trailing = tuple(field.shape[3:])
    half_row, half_column = WLAT // 2, WLON // 2
    shaped = field.reshape(
        (levels, row_count // half_row, half_row, column_count // half_column, half_column)
        + trailing
    )
    order = (1, 3, 0, 2, 4) + tuple(range(5, 5 + len(trailing)))
    return jnp.transpose(shaped, order).reshape(
        (-1, levels * half_row * half_column) + trailing
    )


def from_atoms(atoms, levels, row_count, column_count):
    trailing = tuple(atoms.shape[2:])
    half_row, half_column = WLAT // 2, WLON // 2
    shaped = atoms.reshape(
        (row_count // half_row, column_count // half_column, levels, half_row, half_column)
        + trailing
    )
    order = (2, 0, 3, 1, 4) + tuple(range(5, 5 + len(trailing)))
    return jnp.transpose(shaped, order).reshape((levels, row_count, column_count) + trailing)


def per_device(
    tokens, region, norm_gain1, qkv_weight, proj_weight, norm_gain2, up_weight, down_weight
):
    levels, row_count, column_count, features = tokens.shape
    hidden = up_weight.shape[2]
    x = to_atoms(tokens)
    atoms, size, _ = x.shape
    span = 4 * size

    level = jnp.arange(levels, dtype=jnp.int32)[:, None, None]
    row = (lax.axis_index("lat") * row_count + jnp.arange(row_count, dtype=jnp.int32))[None, :, None]
    pair_first = level // WLEV
    rolled_level = (level + levels - WLEV // 2) % levels
    wrapped_level = (rolled_level >= levels - WLEV // 2).astype(jnp.int32)
    wrapped_row = (row < WLAT // 2).astype(jnp.int32)
    first_class = region * 2 + pair_first
    second_class = ((region * 2 + rolled_level // WLEV) * 2 + wrapped_level) * 2 + wrapped_row
    classes = jnp.stack([first_class, second_class + 64], axis=-1)
    classes = to_atoms(classes)
    lane = jnp.arange(128, dtype=jnp.int32)
    marks = (
        (classes[:, :, :1] == lane) | (classes[:, :, 1:] == lane)
    ).astype(BF16)

    vmem = pl.BlockSpec(memory_space=pltpu.VMEM)
    hbm = pl.BlockSpec(memory_space=pl.ANY)
    out = pl.pallas_call(
        kernel,
        out_shape=jax.ShapeDtypeStruct((atoms, size, features), BF16),
        in_specs=[vmem] * 4 + [hbm] * 4,
        out_specs=vmem,
        scratch_shapes=[
            pltpu.VMEM((atoms, size, features), BF16),
            pltpu.VMEM((2, 4, size, features), BF16),
            pltpu.VMEM((2, 4, size, features), BF16),
            pltpu.VMEM((2, 4, size, 128), BF16),
            pltpu.VMEM((4, span, features), F32),
            pltpu.VMEM((4, span, 3 * features), BF16),
            pltpu.VMEM((4, span, features), BF16),
            pltpu.VMEM((4, span, span), F32),
            pltpu.VMEM(qkv_weight.shape, BF16),
            pltpu.VMEM(proj_weight.shape, BF16),
            pltpu.VMEM(up_weight.shape, BF16),
            pltpu.VMEM(down_weight.shape, BF16),
            pltpu.SemaphoreType.DMA((8,)),
            pltpu.SemaphoreType.DMA((5,)),
            pltpu.SemaphoreType.DMA((5,)),
            pltpu.SemaphoreType.DMA((5,)),
            pltpu.SemaphoreType.DMA((5,)),
            pltpu.SemaphoreType.DMA((5,)),
            pltpu.SemaphoreType.DMA((5,)),
        ],
        compiler_params=pltpu.CompilerParams(
            collective_id=0, has_side_effects=True, vmem_limit_bytes=50 * 1024 * 1024
        ),
    )(x, marks, norm_gain1, norm_gain2, qkv_weight, proj_weight, up_weight, down_weight)
    return from_atoms(out, levels, row_count, column_count)


def solution(mesh):
    return jax.shard_map(
        per_device,
        mesh=mesh,
        in_specs=(P(None, "lat", "lon", None), P(None, "lat", "lon"), P(), P(), P(), P(), P(), P()),
        out_specs=P(None, "lat", "lon", None),
        check_vma=False,
    )
```

```python
import functools

import jax
import jax.numpy as jnp
from jax import lax
from jax.experimental import pallas as pl
from jax.experimental.pallas import tpu as pltpu
from jax.sharding import PartitionSpec as P

HEADS = 8
WLEV = 2
WLAT = 6
WLON = 12
EPSILON = 1e-05
FAR = -1e30
MESH = pl.DeviceIdType.MESH
F32 = jnp.float32
BF16 = jnp.bfloat16


def normed(field, gain):
    mean = jnp.mean(field, axis=-1, keepdims=True)
    centered = field - mean
    variance = jnp.mean(centered * centered, axis=-1, keepdims=True)
    return (centered * lax.rsqrt(variance + EPSILON) * gain).astype(BF16)


def gelu(x):
    inner = x * (0.7978845608028654 + 0.035677408136300125 * (x * x))
    half = 0.5 * x
    return half + half * jnp.tanh(inner)


def dot(a, b):
    return jnp.dot(a, b, preferred_element_type=F32)


def dot_t(a, b):
    return lax.dot_general(a, b, (((1,), (1,)), ((), ())), preferred_element_type=F32)


def kernel(
    x_ref, e_ref, g1_ref, g2_ref, wqkv_hbm, wproj_hbm, wup_hbm, wdown_hbm, out_ref,
    own, shift, back, eshift, xs, qkv, heads, bias,
    wqkv, wproj, wup, wdown, wsem, fsend, frecv, bsend, brecv, esend, erecv,
):
    lat_count, lon_count = lax.axis_size("lat"), lax.axis_size("lon")
    lat, lon = lax.axis_index("lat"), lax.axis_index("lon")
    up = lax.rem(lat + lat_count - 1, lat_count)
    down = lax.rem(lat + 1, lat_count)
    left = lax.rem(lon + lon_count - 1, lon_count)
    right = lax.rem(lon + 1, lon_count)
    before = {"left": (lat, left), "up": (up, lon), "corner": (up, left)}
    after = {"left": (lat, right), "up": (down, lon), "corner": (down, right)}

    weights = [
        pltpu.make_async_copy(source.at[block], target.at[block], wsem.at[block * 4 + at])
        for block in range(2)
        for at, (source, target) in enumerate(
            ((wqkv_hbm, wqkv), (wproj_hbm, wproj), (wup_hbm, wup), (wdown_hbm, wdown))
        )
    ]
    weights[0].start()
    weights[1].start()

    barrier = pltpu.get_barrier_semaphore()
    for device in list(before.values()) + list(after.values()):
        pl.semaphore_signal(barrier, inc=1, device_id=device, device_id_type=MESH)

    moves = (
        (2, 0, 0, "left"),
        (0, 1, 1, "corner"),
        (4, 0, 1, "left"),
        (6, 1, 0, "left"),
        (1, 1, 2, "up"),
    )
    local = {(0, 2): 3, (0, 3): 5, (1, 3): 7}
    arrivals = {(move[1], move[2]): at for at, move in enumerate(moves)}

    def label_copy(at):
        atom, window, place, towards = moves[at]
        return pltpu.make_async_remote_copy(
            e_ref.at[atom], eshift.at[window, place], esend.at[at], erecv.at[at],
            device_id=before[towards], device_id_type=MESH,
        )

    def forward_copy(at):
        atom, window, place, towards = moves[at]
        return pltpu.make_async_remote_copy(
            own.at[atom], shift.at[window, place], fsend.at[at], frecv.at[at],
            device_id=before[towards], device_id_type=MESH,
        )

    row_count, chunk = back.shape[2:4]

    def home(atom):
        return out_ref.at[
            pl.ds(atom // 2 * row_count, row_count), pl.ds(atom % 2 * chunk, chunk), :
        ]

    def backward_copy(at):
        atom, window, place, towards = moves[at]
        return pltpu.make_async_remote_copy(
            back.at[window, place], home(atom), bsend.at[at], brecv.at[at],
            device_id=after[towards], device_id_type=MESH,
        )

    span, features = xs.shape[1:]
    atom_size = span // 4
    part_size = span // 2
    pair = 128
    lane = lax.broadcasted_iota(jnp.int32, (1, pair), 1)
    low = lane < 64
    scale = 64 ** -0.5
    head_masks = (
        jnp.where(low, scale, 0.0).astype(BF16),
        jnp.where(low, 0.0, scale).astype(BF16),
    )

    def prepare(block, at, pieces, marks):
        index = 2 * block + at
        marks = jnp.concatenate([piece.astype(F32) for piece in marks], axis=0)
        half = low if block == 0 else jnp.logical_not(low)
        query = (marks * jnp.where(half, FAR, 0.0)).astype(BF16)
        bias[index] = dot_t(query, (1.0 - marks).astype(BF16))
        x = jnp.concatenate([piece.astype(F32) for piece in pieces], axis=0)
        xs[index] = x
        n1 = normed(x, g1_ref[block : block + 1, :])
        if at == 0:
            weights[block * 4].wait()
        qkv[index] = dot(n1, wqkv[block]).astype(BF16)

    def part(block, at, which, first):
        index = 2 * block + at
        rows = slice(which * part_size, (which + 1) * part_size)
        ones = jnp.ones((span, pair), BF16)
        offset = bias[index, rows, :]
        offset = jnp.concatenate([offset, offset], axis=0)
        for column in range(0, features, pair):
            query = qkv[index, rows, column : column + pair]
            key = qkv[index, :, features + column : features + column + pair]
            value = qkv[index, :, 2 * features + column : 2 * features + column + pair]
            value = jnp.concatenate([value, ones], axis=1)
            query = jnp.concatenate([query * head_masks[0], query * head_masks[1]], axis=0)
            scores = dot_t(query, key) + offset
            peak = jnp.max(scores, axis=-1, keepdims=True)
            weight = jnp.exp(scores - peak).astype(BF16)
            total = dot(weight, value)
            total = total[:, :pair] / total[:, pair:]
            heads[index, rows, column : column + pair] = jnp.where(
                low, total[:part_size], total[part_size:]
            ).astype(BF16)
        if first:
            weights[block * 4 + 1].wait()
        h = xs[index, rows, :] + dot(heads[index, rows, :], wproj[block])
        n2 = normed(h, g2_ref[block : block + 1, :])
        if first:
            weights[block * 4 + 2].wait()
            weights[block * 4 + 3].wait()
        hidden = wup.shape[2]
        step = 512
        for column in range(0, hidden, step):
            inner = gelu(dot(n2, wup[block, :, column : column + step])).astype(BF16)
            h = h + dot(inner, wdown[block, column : column + step, :])
        return h[:atom_size], h[atom_size:]

    def prepare_first(u):
        atoms = (4 * u, 4 * u + 2, 4 * u + 1, 4 * u + 3)
        pieces = [
            x_ref[a // 2 * row_count + row, a % 2 * chunk : (a % 2 + 1) * chunk, :]
            for a in atoms
            for row in range(row_count)
        ]
        prepare(0, u, pieces, [e_ref[a] for a in atoms])

    def part_first(u, which, first=False):
        results = part(0, u, which, first)
        own[4 * u + which] = results[0].astype(BF16)
        own[4 * u + 2 + which] = results[1].astype(BF16)

    prepare_first(0)
    weights[2].start()
    weights[3].start()
    part_first(0, 0, True)
    pl.semaphore_wait(barrier, 6)
    for at in range(5):
        label_copy(at).start()
    forward_copy(0).start()
    for at in range(4, 8):
        weights[at].start()
    prepare_first(1)
    part_first(1, 0)
    forward_copy(2).start()
    forward_copy(1).start()
    forward_copy(3).start()
    part_first(0, 1)
    forward_copy(4).start()
    part_first(1, 1)

    def prepare_second(w):
        pieces, marks = [], []
        for place in range(4):
            if (w, place) in arrivals:
                label_copy(arrivals[w, place]).wait_recv()
                forward_copy(arrivals[w, place]).wait_recv()
        for place in range(4):
            if (w, place) in arrivals:
                pieces.append(shift[w, place])
                marks.append(eshift[w, place])
            else:
                pieces.append(own[local[w, place]])
                marks.append(e_ref[local[w, place]])
        prepare(1, w, pieces, marks)

    def part_second(w, which, first=False):
        results = part(1, w, which, first)
        for at in range(2):
            place = 2 * which + at
            for row in range(row_count):
                piece = results[at][row * chunk : (row + 1) * chunk].astype(BF16)
                if (w, place) in local:
                    atom = local[w, place]
                    out_ref[
                        atom // 2 * row_count + row, atom % 2 * chunk : (atom % 2 + 1) * chunk, :
                    ] = piece
                else:
                    back[w, place, row] = piece
        for at in range(2):
            if (w, 2 * which + at) in arrivals:
                backward_copy(arrivals[w, 2 * which + at]).start()

    prepare_second(0)
    part_second(0, 0, True)
    prepare_second(1)
    part_second(1, 0)
    part_second(1, 1)
    part_second(0, 1)
    for at in range(5):
        backward_copy(at).wait_recv()
    for at in range(5):
        label_copy(at).wait_send()
        forward_copy(at).wait_send()
        backward_copy(at).wait_send()


def per_device(
    tokens, region, norm_gain1, qkv_weight, proj_weight, norm_gain2, up_weight, down_weight
):
    levels, row_count, column_count, features = tokens.shape
    half_row, half_column = WLAT // 2, WLON // 2
    groups, halves = row_count // half_row, column_count // half_column
    atoms, chunk = groups * halves, half_column * levels
    size = half_row * chunk
    span = 4 * size
    x = jnp.transpose(tokens, (1, 2, 0, 3)).reshape(row_count, column_count * levels, features)

    region = jnp.transpose(region, (1, 2, 0)).reshape(groups, half_row, halves, chunk)
    region = jnp.transpose(region, (0, 2, 1, 3)).reshape(atoms, size, 1)
    shape = (atoms, size, 128)
    level = lax.broadcasted_iota(jnp.int32, shape, 1) % levels
    rolled_level = (level + levels - WLEV // 2) % levels
    wrapped_level = (rolled_level >= levels - WLEV // 2).astype(jnp.int32)
    top = lax.broadcasted_iota(jnp.int32, shape, 0) < halves
    wrapped_row = (top & (lax.axis_index("lat") == 0)).astype(jnp.int32)
    first_class = region * 2 + level // WLEV
    second_class = ((region * 2 + rolled_level // WLEV) * 2 + wrapped_level) * 2 + wrapped_row
    lane = lax.broadcasted_iota(jnp.int32, shape, 2)
    marks = ((lane == first_class) | (lane == second_class + 64)).astype(BF16)

    vmem = pl.BlockSpec(memory_space=pltpu.VMEM)
    hbm = pl.BlockSpec(memory_space=pl.ANY)
    out = pl.pallas_call(
        kernel,
        out_shape=jax.ShapeDtypeStruct(x.shape, BF16),
        in_specs=[vmem] * 4 + [hbm] * 4,
        out_specs=vmem,
        scratch_shapes=[
            pltpu.VMEM((atoms, size, features), BF16),
            pltpu.VMEM((2, 4, size, features), BF16),
            pltpu.VMEM((2, 4, half_row, chunk, features), BF16),
            pltpu.VMEM((2, 4, size, 128), BF16),
            pltpu.VMEM((4, span, features), F32),
            pltpu.VMEM((4, span, 3 * features), BF16),
            pltpu.VMEM((4, span, features), BF16),
            pltpu.VMEM((4, span, span), F32),
            pltpu.VMEM(qkv_weight.shape, BF16),
            pltpu.VMEM(proj_weight.shape, BF16),
            pltpu.VMEM(up_weight.shape, BF16),
            pltpu.VMEM(down_weight.shape, BF16),
            pltpu.SemaphoreType.DMA((8,)),
            pltpu.SemaphoreType.DMA((5,)),
            pltpu.SemaphoreType.DMA((5,)),
            pltpu.SemaphoreType.DMA((5,)),
            pltpu.SemaphoreType.DMA((5,)),
            pltpu.SemaphoreType.DMA((5,)),
            pltpu.SemaphoreType.DMA((5,)),
        ],
        compiler_params=pltpu.CompilerParams(
            collective_id=0, has_side_effects=True, vmem_limit_bytes=50 * 1024 * 1024
        ),
    )(x, marks, norm_gain1, norm_gain2, qkv_weight, proj_weight, up_weight, down_weight)
    out = out.reshape(row_count, column_count, levels, features)
    return jnp.transpose(out, (2, 0, 1, 3))


def solution(mesh):
    return jax.shard_map(
        per_device,
        mesh=mesh,
        in_specs=(P(None, "lat", "lon", None), P(None, "lat", "lon"), P(), P(), P(), P(), P(), P()),
        out_specs=P(None, "lat", "lon", None),
        check_vma=False,
    )
```
